512 devices in a mesh: seq: 128 (over z, y, core), batch: 4 (over x).
Axes of the slice: x: 4, y: 8, z: 8, core: 2. Of those that a mesh axis runs over, the one named last changes fastest.
Arguments:
- tokens: bfloat16 [4, 131072, 1024], P('batch', 'seq'), may hold values from -24 to 24
- logits: bfloat16 [4, 131072, 256], P('batch', 'seq'), may hold values from -160 to 160
- slot_grad: bfloat16 [4, 256, 1024], P('batch', 'seq'), may hold values from -6 to 6
- phi_param: bfloat16 [1024, 256], P('seq'), may hold values from -0.1875 to 0.1875
Outputs:
- token_grad: bfloat16 [4, 131072, 1024], P('batch', 'seq')
- phi_grad: float32 [1024, 256], P('seq')
The draws below stay inside these ranges and needn't reach their ends.
All inputs are finite; a program needn't handle non-finite values.
Results may differ from the reference program's by a relative error of at most 0.0049.
Values may be sent and summed in bfloat16 or wider, within the bound.
A program may use at most 64 MiB of HBM per device.

```python
import jax
import jax.numpy as jnp
from jax import lax

D = 1024
SLOTS = 256
TOK_DEV = 1024
SEQ_TOKENS = 131072
BATCH = 4


def draw_logits(key, part):
    key_base = jax.random.fold_in(key, 0)
    key_tilt = jax.random.fold_in(key, 1)
    key_offset = jax.random.fold_in(key, 3)
    block_count = SEQ_TOKENS // TOK_DEV
    values = jnp.clip(jax.random.normal(key_base, (BATCH, SEQ_TOKENS, SLOTS), jnp.float32), -6.0, 6.0) * 1.5
    block_tilt = jax.random.uniform(key_tilt, (BATCH, block_count, 1, SLOTS), jnp.float32, -2.0, 2.0)
    values = (values.reshape(BATCH, block_count, TOK_DEV, SLOTS) + block_tilt).reshape(BATCH, SEQ_TOKENS, SLOTS)
    offset = jax.random.uniform(key_offset, (SLOTS,), jnp.float32, -3.0, 3.0)
    values = values + offset
    return jnp.clip(values, -160.0, 160.0).astype(jnp.bfloat16)


def spiked(entries, key, source, target, parts, factor):
    def block_of(axis_at):
        return (jnp.arange(entries.shape[axis_at]) // (entries.shape[axis_at] // parts)).reshape((-1,) + (1,) * (entries.ndim - 1 - axis_at))

    one_side = jax.random.permutation(key, parts)[block_of(target)]
    other_side = (block_of(target) + parts // 2) % parts
    return jnp.where((block_of(source) == one_side) | (block_of(source) == other_side), factor * entries, entries)


def steps_of(rng, shape, shards, smallest, top_value):
    level = 1.0
    for position, parts in shards:
        steps = jax.random.uniform(jax.random.fold_in(jax.random.fold_in(rng, 6), position), (parts,), jnp.float32, smallest / len(shards), top_value / len(shards))
        level = level * jnp.repeat(jnp.exp(steps), shape[position] // parts).reshape((-1,) + (1,) * (len(shape) - 1 - position))
    return level


def scatter_about(rng, dims, spread, most, cuts=(), kind=jnp.bfloat16):
    drawn = spread * jax.random.normal(rng, dims, jnp.float32)
    if cuts:
        drawn = drawn * steps_of(rng, dims, cuts, -0.22, 0.18)
    return jnp.clip(drawn, -most, most).astype(kind)


def gaussian_with(rng, extent, deviation, bound, pieces, heavy, held_as=jnp.bfloat16):
    drawn = deviation * jax.random.normal(rng, extent, jnp.float32)
    if pieces:
        drawn = drawn * steps_of(rng, extent, pieces, -0.22, 0.18)
    return jnp.clip(spiked(drawn, jax.random.fold_in(rng, 3), *heavy), -bound, bound).astype(held_as)


def setup_inputs(seed: int = 0) -> dict:
    arg_keys = jax.random.split(jax.random.key(seed), 5)
    tokens = gaussian_with(arg_keys[0], (BATCH, SEQ_TOKENS, D), 1.0, 24.0, ((0, 4), (1, 128)), (1, 2, 128, 5.5))
    logits = draw_logits(jax.random.fold_in(arg_keys[4], 71), 0)
    slot_grad = scatter_about(arg_keys[2], (BATCH, SLOTS, D), 1.0, 6.0, ((0, 4), (1, 128)))
    phi_param = scatter_about(arg_keys[3], (D, SLOTS), D ** -0.5, 0.1875, ((0, 128),))
    return dict(tokens=tokens, logits=logits, slot_grad=slot_grad, phi_param=phi_param)


def reference(tokens, logits, slot_grad, phi_param):
    grad_scale = float(SEQ_TOKENS // 16)
    phi_grad = jnp.zeros((D, SLOTS), jnp.float32)
    results = []
    for seq_index in range(BATCH):
        inputs = tokens[seq_index]
        scores = logits[seq_index].astype(jnp.float32)
        upstream = slot_grad[seq_index]
        col_peak = jnp.max(scores, axis=0, keepdims=True)
        raw_weights = jnp.exp(scores - col_peak)
        col_total = jnp.sum(raw_weights, axis=0, keepdims=True)
        dispatch = raw_weights / col_total
        weight_grad = lax.dot_general(inputs, upstream, (((1,), (1,)), ((), ())), preferred_element_type=jnp.float32)
        col_dot = jnp.sum(dispatch * weight_grad, axis=0, keepdims=True)
        logit_grad = (dispatch * (weight_grad - col_dot)).astype(jnp.bfloat16)
        dispatch_low = dispatch.astype(jnp.bfloat16)
        token_sum = jnp.dot(dispatch_low, upstream, preferred_element_type=jnp.float32)
        token_sum = token_sum + lax.dot_general(logit_grad, phi_param, (((1,), (1,)), ((), ())), preferred_element_type=jnp.float32)
        results.append((grad_scale * token_sum).astype(jnp.bfloat16))
        phi_grad = phi_grad + lax.dot_general(inputs, logit_grad, (((0,), (0,)), ((), ())), preferred_element_type=jnp.float32)
    return jnp.stack(results), phi_grad
```

```python
import functools

import jax
import jax.numpy as jnp
from jax import lax
from jax.experimental import pallas as pl
from jax.experimental.pallas import tpu as pltpu
from jax.sharding import Mesh
from jax.sharding import PartitionSpec as P

SEQ = ("seq_0", "seq_1", "seq_2")
MESH = pl.DeviceIdType.MESH
F32 = jnp.float32
BF16 = jnp.bfloat16
NT = (((1,), (1,)), ((), ()))


def ring_order(n):
    return sorted(range(1, n), key=lambda k: (-min(k, n - k), k))


def kernel(
    sizes, tok_h, log_h, g_h, phi_h, tg_h, pg_o,
    tok, tokT, logv, gy, py, gall, pall, p, wg, st, sa, sb, dlow, lg,
    own, dsnd, drcv, zsnd, zrcv, ysnd, yrcv, xbuf, tgv,
    lsem, ssem, rsem, gsem, csem, osem,
):
    nz, ny, nc, nx = sizes
    z, y, c, x = (lax.axis_index(a) for a in (*SEQ, "batch"))
    ts, d = tok.shape
    slots = logv.shape[1]
    half = d // 2
    rank = y * nc + c
    n16 = ny * nc
    tile = min(256, ts)
    other = nc - 1 - c

    def row_peer(j):
        i = lax.rem(rank + j, n16)
        return (z, lax.div(i, nc), lax.rem(i, nc), x)

    def z_peer(k):
        return (lax.rem(z + k, nz), y, c, x)

    def y_peer(k):
        return (z, lax.rem(y + k, ny), c, x)

    def x_peer(k):
        return (z, y, c, lax.rem(x + k, nx))

    partner = (z, y, other, x)

    def send(src, dst, s, r, to):
        pltpu.make_async_remote_copy(
            src_ref=src, dst_ref=dst, send_sem=s, recv_sem=r, device_id=to, device_id_type=MESH
        ).start()

    def await_bytes(ref, sem):
        pltpu.make_async_copy(ref, ref, sem).wait()

    loads = [
        pltpu.make_async_copy(g_h, gy.at[rank], lsem.at[0]),
        pltpu.make_async_copy(phi_h, py.at[rank], lsem.at[1]),
        pltpu.make_async_copy(log_h, logv, lsem.at[2]),
        pltpu.make_async_copy(tok_h, tok, lsem.at[3]),
    ]
    for one in loads:
        one.start()

    barrier = pltpu.get_barrier_semaphore()
    peers = [row_peer(j) for j in range(1, n16)]
    peers += [z_peer(k) for k in range(1, nz)] + [x_peer(k) for k in range(1, nx)]
    for to in peers:
        pl.semaphore_signal(barrier, inc=1, device_id=to, device_id_type=MESH)
    loads[0].wait()
    loads[1].wait()
    pl.semaphore_wait(barrier, len(peers))

    for j in range(1, n16):
        send(gy.at[rank], gy.at[rank], ssem.at[0], rsem.at[0], row_peer(j))
    for j in range(1, n16):
        send(py.at[rank], py.at[rank], ssem.at[1], rsem.at[1], row_peer(j))

    loads[2].wait()
    scores = logv[...].astype(F32)
    peak = jnp.max(scores, axis=0, keepdims=True)
    raw = jnp.exp(scores - peak)
    p[...] = raw
    total = jnp.sum(raw, axis=0, keepdims=True)

    await_bytes(gy.at[pl.ds(0, n16 - 1)], rsem.at[0])
    block = jnp.concatenate([gy[i].astype(F32) for i in range(n16)], axis=0).astype(BF16)
    gall[0, z] = block[:, :half]
    gall[1, z] = block[:, half:]
    order = ring_order(nz)
    for k in order:
        send(gall.at[c, z], gall.at[c, z], ssem.at[2], gsem.at[k - 1], z_peer(k))

    loads[3].wait()
    dt = min(128, d)

    def turn(i, carry):
        r = pl.ds(pl.multiple_of(i * dt, dt), dt)
        tokT[r, :] = tok[:, r].T
        return carry

    lax.fori_loop(0, d // dt, turn, 0)

    for k in reversed(order):
        src = lax.rem(z + nz - k, nz)
        await_bytes(gall.at[c, src], gsem.at[k - 1])
        send(gall.at[c, src], gall.at[c, src], ssem.at[3], rsem.at[2], partner)
    await_bytes(gall.at[other, pl.ds(0, nz - 1)], rsem.at[2])

    g0 = gall[0].reshape(slots, half)
    g1 = gall[1].reshape(slots, half)

    def weigh(i, acc):
        r = pl.ds(pl.multiple_of(i * tile, tile), tile)
        t = tok[r, :]
        w = lax.dot_general(t[:, :half], g0, NT, preferred_element_type=F32)
        w = w + lax.dot_general(t[:, half:], g1, NT, preferred_element_type=F32)
        wg[r, :] = w
        return acc + jnp.sum(p[r, :] * w, axis=0, keepdims=True)

    dots = lax.fori_loop(0, ts // tile, weigh, jnp.zeros((1, slots), F32))

    def merged(parts):
        top = functools.reduce(jnp.maximum, [a[0:1] for a in parts])
        scale = [jnp.exp(a[0:1] - top) for a in parts]
        one = sum(a[1:2] * s for a, s in zip(parts, scale))
        two = sum(a[2:3] * s for a, s in zip(parts, scale))
        return jnp.concatenate([top, one, two, jnp.zeros_like(top)], axis=0)

    mine = jnp.concatenate([peak, total, dots, jnp.zeros_like(dots)], axis=0)
    st[0] = mine
    for k in order:
        send(st.at[0], sa.at[k - 1], ssem.at[4], rsem.at[3], z_peer(k))

    hb = n16 // 2
    await_bytes(py.at[pl.ds(0, n16 - 1)], rsem.at[1])
    pall[z] = py[...]
    for k in order:
        part = pl.ds(c * hb, hb)
        send(pall.at[z, part], pall.at[z, part], ssem.at[5], gsem.at[nz - 1 + k - 1], z_peer(k))

    await_bytes(sa, rsem.at[3])
    mine = merged([mine] + [sa[k] for k in range(nz - 1)])
    st[1] = mine
    for j in range(1, n16):
        send(st.at[1], sb.at[j - 1], ssem.at[6], rsem.at[4], row_peer(j))
    await_bytes(sb, rsem.at[4])
    mine = merged([mine] + [sb[k] for k in range(n16 - 1)])
    scale = jnp.exp(peak - mine[0:1]) / mine[1:2]
    center = mine[2:3] / mine[1:2]

    def grade(i, carry):
        r = pl.ds(pl.multiple_of(i * tile, tile), tile)
        dispatch = p[r, :] * scale
        dlow[r, :] = dispatch.astype(BF16)
        lg[r, :] = (dispatch * (wg[r, :] - center)).astype(BF16)
        return carry

    lax.fori_loop(0, ts // tile, grade, 0)

    rb = d // (nz * n16)
    zb = n16 * rb
    chunks = [*order, 0]
    for q, k in enumerate(chunks):
        to = lax.rem(z + k, nz)
        r = pl.ds(pl.multiple_of(to * zb, zb), zb)
        res = jnp.dot(tokT[r, :], lg[...], preferred_element_type=F32)
        res = res.reshape(ny, 2, rb, slots)
        keep = jnp.where(c == 0, res[:, 0], res[:, 1])
        give = jnp.where(c == 0, res[:, 1], res[:, 0])
        own[q] = keep.reshape(ny * rb, slots)
        dsnd[q] = give.reshape(ny * rb, slots).astype(BF16)
        send(dsnd.at[q], drcv.at[q], ssem.at[7], csem.at[q], partner)
    for q, k in enumerate(chunks):
        await_bytes(drcv.at[q], csem.at[q])
        both = own[q] + drcv[q].astype(F32)
        if k:
            zsnd[q] = both.astype(BF16)
            send(zsnd.at[q], zrcv.at[k - 1], ssem.at[8], rsem.at[5], z_peer(k))
        else:
            own[q] = both

    for k in reversed(order):
        src = lax.rem(z + nz - k, nz)
        part = pl.ds(c * hb, hb)
        await_bytes(pall.at[src, part], gsem.at[nz - 1 + k - 1])
        send(pall.at[src, part], pall.at[src, part], ssem.at[9], rsem.at[6], partner)
    await_bytes(pall.at[pl.ds(0, nz - 1), pl.ds(0, hb)], rsem.at[6])
    grad_scale = float(ts * nz * n16 // 16)

    def emit(i, carry):
        r = pl.ds(pl.multiple_of(i * tile, tile), tile)
        for h in range(2):
            g = gall[h].reshape(slots, half)
            ph = pall[h * nz // 2 : (h + 1) * nz // 2].astype(F32).reshape(half, slots).astype(BF16)
            s = jnp.dot(dlow[r, :], g, preferred_element_type=F32)
            s = s + lax.dot_general(lg[r, :], ph, NT, preferred_element_type=F32)
            tgv[r, h * half : (h + 1) * half] = (grad_scale * s).astype(BF16)
        pltpu.make_async_copy(tgv.at[r], tg_h.at[r], osem.at[i]).start()
        return carry

    lax.fori_loop(0, ts // tile, emit, 0)

    await_bytes(zrcv, rsem.at[5])
    acc = own[nz - 1]
    for k in range(nz - 1):
        acc = acc + zrcv[k].astype(F32)
    ysnd[...] = acc.reshape(ny, rb, slots)
    yorder = ring_order(ny)
    for k in yorder:
        send(ysnd.at[lax.rem(y + k, ny)], yrcv.at[k - 1], ssem.at[10], rsem.at[7], y_peer(k))
    acc = ysnd[y]
    await_bytes(yrcv, rsem.at[7])
    for k in range(ny - 1):
        acc = acc + yrcv[k]
    xbuf[x] = acc
    for k in ring_order(nx):
        send(xbuf.at[x], xbuf.at[x], ssem.at[11], rsem.at[8], x_peer(k))
    await_bytes(xbuf.at[pl.ds(0, nx - 1)], rsem.at[8])
    acc = xbuf[0]
    for k in range(1, nx):
        acc = acc + xbuf[k]
    pg_o[...] = acc

    await_bytes(gy.at[pl.ds(0, n16 - 1)], ssem.at[0])
    await_bytes(py.at[pl.ds(0, n16 - 1)], ssem.at[1])
    await_bytes(gall.at[0, pl.ds(0, nz - 1)], ssem.at[2])
    await_bytes(gall.at[0, pl.ds(0, nz - 1)], ssem.at[3])
    await_bytes(sa, ssem.at[4])
    await_bytes(pall.at[pl.ds(0, nz - 1), pl.ds(0, hb)], ssem.at[5])
    await_bytes(sb, ssem.at[6])
    await_bytes(drcv, ssem.at[7])
    await_bytes(zrcv, ssem.at[8])
    await_bytes(pall.at[pl.ds(0, nz - 1), pl.ds(0, hb)], ssem.at[9])
    await_bytes(yrcv, ssem.at[10])
    await_bytes(xbuf.at[pl.ds(0, nx - 1)], ssem.at[11])
    for i in range(ts // tile):
        r = pl.ds(i * tile, tile)
        pltpu.make_async_copy(tgv.at[r], tg_h.at[r], osem.at[i]).wait()


def per_device(sizes, tokens, logits, slot_grad, phi_param):
    nz, ny, nc, nx = sizes
    tokens, logits, slot_grad = tokens[0], logits[0], slot_grad[0]
    ts, d = tokens.shape
    slots = logits.shape[1]
    n16 = ny * nc
    rb = d // (nz * n16)
    sl = slots // (nz * n16)
    half = d // 2
    tile = min(256, ts)
    vm, dma = pltpu.VMEM, pltpu.SemaphoreType.DMA
    any_spec = pl.BlockSpec(memory_space=pl.ANY)
    scratch = [
        vm((ts, d), BF16), vm((d, ts), BF16), vm((ts, slots), BF16),
        vm((n16, sl, d), BF16), vm((n16, rb, slots), BF16),
        vm((2, nz, n16 * sl, half), BF16), vm((nz, n16, rb, slots), BF16),
        vm((ts, slots), F32), vm((ts, slots), F32),
        vm((2, 4, slots), F32), vm((nz - 1, 4, slots), F32), vm((n16 - 1, 4, slots), F32),
        vm((ts, slots), BF16), vm((ts, slots), BF16),
        vm((nz, ny * rb, slots), F32), vm((nz, ny * rb, slots), BF16), vm((nz, ny * rb, slots), BF16),
        vm((nz - 1, ny * rb, slots), BF16), vm((nz - 1, ny * rb, slots), BF16),
        vm((ny, rb, slots), F32), vm((ny - 1, rb, slots), F32),
        vm((nx, rb, slots), F32), vm((ts, d), BF16),
        dma((4,)), dma((12,)), dma((9,)), dma((2 * (nz - 1),)), dma((nz,)), dma((ts // tile,)),
    ]
    token_grad, phi_grad = pl.pallas_call(
        functools.partial(kernel, sizes),
        out_shape=(
            jax.ShapeDtypeStruct((ts, d), BF16),
            jax.ShapeDtypeStruct((rb, slots), F32),
        ),
        in_specs=[any_spec] * 4,
        out_specs=(any_spec, pl.BlockSpec(memory_space=pltpu.VMEM)),
        scratch_shapes=scratch,
        compiler_params=pltpu.CompilerParams(
            collective_id=0, has_side_effects=True, vmem_limit_bytes=48 * 1024 * 1024
        ),
        name="moe_dispatch_backward",
    )(tokens, logits, slot_grad, phi_param)
    return token_grad[None], phi_grad


def solution(mesh):
    shape = mesh.devices.shape
    nc = 2
    ny = 8 if shape[0] % 128 == 0 else 2
    sizes = (shape[0] // (ny * nc), ny, nc, shape[1])
    finer = Mesh(mesh.devices.reshape(sizes), (*SEQ, "batch"))
    in_specs = (P("batch", SEQ, None), P("batch", SEQ, None), P("batch", SEQ, None), P(SEQ, None))
    out_specs = (P("batch", SEQ, None), P(SEQ, None))
    return jax.shard_map(
        functools.partial(per_device, sizes),
        mesh=finer, in_specs=in_specs, out_specs=out_specs, check_vma=False,
    )
```

```python
import contextlib
import functools

import jax
import jax.numpy as jnp
from jax import lax
from jax.experimental import pallas as pl
from jax.experimental.pallas import tpu as pltpu
from jax.sharding import Mesh
from jax.sharding import PartitionSpec as P

SEQ = ("seq_0", "seq_1", "seq_2")
MESH = pl.DeviceIdType.MESH
F32 = jnp.float32
BF16 = jnp.bfloat16
NT = (((1,), (1,)), ((), ()))


def far_first(n):
    return sorted(range(1, n), key=lambda k: (-min(k, n - k), k))


def kernel(
    n, nx, tok_h, log_h, g_h, phi_h, tg_o, pg_o,
    tok, tokT, logv, p, wg, dr, u, w, phim,
    g_other, p_other, l1, gh, ph, st_a, st_m, st_b,
    asnd, arcv, bsnd, brcv, bsum, r, rrcv, xs, xbuf, tgs, tgr,
    lsem, ssem, rsem, osem,
):
    open_scope = contextlib.ExitStack()

    def phase(name):
        open_scope.close()
        open_scope.enter_context(jax.named_scope(name))

    phase("greet")
    z, y, c, x = (lax.axis_index(a) for a in (*SEQ, "batch"))
    other = 1 - c
    a = z * other + y * c
    b = y * other + z * c
    _, ts, d = tok.shape
    sl = logv.shape[2]
    half = d // 2
    rows = d // (n * n)
    tile = min(256, ts)
    order = far_first(n)

    def along_a(k, core):
        return (lax.rem(z + k * other, n), lax.rem(y + k * c, n), core, x)

    def along_b(k, core):
        return (lax.rem(z + k * c, n), lax.rem(y + k * other, n), core, x)

    def along_x(k, core):
        return (z, y, core, lax.rem(x + k, nx))

    partner = (z, y, other, x)

    def send(src, dst, s, q, to):
        pltpu.make_async_remote_copy(
            src_ref=src, dst_ref=dst, send_sem=s, recv_sem=q, device_id=to, device_id_type=MESH
        ).start()

    def await_bytes(ref, sem):
        pltpu.make_async_copy(ref, ref, sem).wait()

    mine = pl.ds(pl.multiple_of(c * half, half), half)
    theirs = pl.ds(pl.multiple_of(other * half, half), half)
    my_slots = pl.ds(pl.multiple_of(c * sl, sl), sl)
    their_slots = pl.ds(pl.multiple_of(other * sl, sl), sl)
    loads = [
        pltpu.make_async_copy(g_h.at[:, mine], l1.at[b, c], lsem.at[0]),
        pltpu.make_async_copy(g_h.at[:, theirs], g_other, lsem.at[1]),
        pltpu.make_async_copy(phi_h.at[:, my_slots], ph.at[a, b, c], lsem.at[2]),
        pltpu.make_async_copy(phi_h.at[:, their_slots], p_other, lsem.at[3]),
        pltpu.make_async_copy(log_h.at[:, my_slots], logv.at[0], lsem.at[4]),
        pltpu.make_async_copy(tok_h, tok.at[0], lsem.at[5]),
    ]
    for one in loads:
        one.start()

    barrier = pltpu.get_barrier_semaphore()
    peers = [partner]
    for core in (c, other):
        for k in range(1, n):
            peers += [along_a(k, core), along_b(k, core)]
        peers += [along_x(k, core) for k in range(1, nx)]
    for to in peers:
        pl.semaphore_signal(barrier, inc=1, device_id=to, device_id_type=MESH)
    loads[0].wait()
    loads[1].wait()
    pl.semaphore_wait(barrier, len(peers))

    phase("g1_send")
    for k in order:
        send(l1.at[b, c], l1.at[b, c], ssem.at[0], rsem.at[0], along_b(k, c))
        send(g_other, l1.at[a, c], ssem.at[1], rsem.at[1], along_a(k, other))
    send(g_other, l1.at[a, c], ssem.at[1], rsem.at[1], partner)
    send(log_h.at[:, their_slots], logv.at[1], ssem.at[2], rsem.at[2], partner)
    loads[2].wait()
    loads[3].wait()
    for k in order:
        send(ph.at[a, b, c], ph.at[a, b, c], ssem.at[3], rsem.at[3], along_b(k, c))
        send(p_other, ph.at[b, a, c], ssem.at[4], rsem.at[4], along_a(k, other))
    send(p_other, ph.at[b, a, c], ssem.at[4], rsem.at[4], partner)
    send(tok_h, tok.at[1], ssem.at[5], rsem.at[5], partner)

    phase("peak")
    loads[4].wait()
    await_bytes(logv.at[1], rsem.at[2])
    peak = jnp.max(logv[...].astype(F32), axis=(0, 1))[None]
    total = jnp.zeros((1, sl), F32)
    for i in range(2):
        raw = jnp.exp(logv[i].astype(F32) - peak)
        p[i] = raw
        total = total + jnp.sum(raw, axis=0, keepdims=True)
    blank = jnp.zeros((2, sl), F32)
    st_a[a] = jnp.concatenate([peak, total, blank], axis=0)
    for k in order:
        send(st_a.at[a], st_a.at[a], ssem.at[6], rsem.at[6], along_a(k, c))

    lanes = n * rows

    def turn(i):
        for j in range(n):
            blk = tok[i, :, j * lanes : (j + 1) * lanes].T
            for m in range(n):
                ja = j * other + m * c
                jb = m * other + j * c
                row = (lax.rem(ja - a + 2 * n - 1, n) * n + jb) * rows
                tokT[pl.ds(pl.multiple_of(row, rows), rows), i * ts : (i + 1) * ts] = blk[
                    m * rows : (m + 1) * rows
                ]

    phase("turn0")
    loads[5].wait()
    turn(0)

    phase("g1_wait")
    await_bytes(l1.at[pl.ds(0, n - 1), 0], rsem.at[0])
    await_bytes(l1.at[:, 0], rsem.at[1])
    nh = n // 2
    near = lax.div(z, nh)
    zz = lax.rem(z, nh)

    @pl.when(c == 0)
    def _():
        for k in order:
            send(l1, gh.at[0, zz], ssem.at[7], rsem.at[7], along_a(k, near))

        @pl.when(near == 0)
        def _():
            pltpu.make_async_copy(l1, gh.at[0, zz], rsem.at[7]).start()

        @pl.when(near == 1)
        def _():
            send(l1, gh.at[0, zz], ssem.at[8], rsem.at[7], partner)

    @pl.when(c == 1)
    def _():
        for k in order:
            for q in range(2):
                send(
                    l1.at[pl.ds(q * nh, nh)], gh.at[1, :, y], ssem.at[7], rsem.at[8],
                    along_a(k, q),
                )
        send(l1.at[pl.ds(0, nh)], gh.at[1, :, y], ssem.at[8], rsem.at[8], partner)
        pltpu.make_async_copy(l1.at[pl.ds(nh, nh)], gh.at[1, :, y], rsem.at[8]).start()

    phase("phi_send")
    await_bytes(ph.at[0, pl.ds(0, n - 1), 0], rsem.at[3])
    await_bytes(ph.at[0, :, 0], rsem.at[4])
    for k in order:
        send(ph.at[a], ph.at[a], ssem.at[9], rsem.at[9], along_a(k, c))

    phase("turn1")
    await_bytes(tok.at[1], rsem.at[5])
    turn(1)

    phase("ml_wait")
    await_bytes(st_a.at[pl.ds(0, n - 1)], rsem.at[6])
    tops = [st_a[i, 0:1] for i in range(n)]
    ring_peak = functools.reduce(jnp.maximum, tops)
    ring_total = sum(st_a[i, 1:2] * jnp.exp(t - ring_peak) for i, t in enumerate(tops))
    to_ring = jnp.exp(peak - ring_peak)

    def weigh_ring(i):
        dr[i * ts : (i + 1) * ts] = (p[i] * to_ring).astype(BF16)

    weigh_ring(0)
    weigh_ring(1)

    blk = n * rows

    def reduce_first(snd, rcv, s, q):
        starts = sorted(range(0, n, 2), key=lambda i: -max(min(i + 1, n - i - 1), min(i + 2, n - i - 2)))
        for start in starts:
            res = jnp.dot(
                tokT[start * blk : (start + 2) * blk], dr[...], preferred_element_type=F32
            )
            for i in sorted(range(start, start + 2), key=lambda i: -min(i + 1, n - i - 1)):
                part = res[(i - start) * blk : (i - start + 1) * blk]
                if i == n - 1:
                    own = part
                else:
                    snd[i] = part.astype(BF16)
                    send(snd.at[i], rcv.at[i], s, q, along_a(i + 1, c))
        return own

    phase("b_send")
    bsum[...] = reduce_first(bsnd, brcv, ssem.at[10], rsem.at[10])

    phase("g2_wait")
    await_bytes(gh.at[0], rsem.at[7])
    await_bytes(gh.at[1], rsem.at[8])
    phase("weigh")
    per = n * 2 * gh.shape[4]
    for h in range(2):
        for i in range(nh):
            parts = [gh[h, i, j, k].astype(F32) for j in range(n) for k in range(2)]
            w[i * per : (i + 1) * per, h * half : (h + 1) * half] = jnp.concatenate(
                parts, axis=0
            ).astype(BF16)

    dots = jnp.zeros((1, sl), F32)
    for i in range(2):

        def weigh(j, acc, i=i):
            at = pl.ds(pl.multiple_of(j * tile, tile), tile)
            v = lax.dot_general(tok[i, at, :], w[0:sl, :], NT, preferred_element_type=F32)
            wg[i, at, :] = v
            return acc + jnp.sum(p[i, at, :] * v, axis=0, keepdims=True)

        dots = lax.fori_loop(0, ts // tile, weigh, dots)

    phase("mean")
    st_m[a] = jnp.concatenate([dots * to_ring, jnp.zeros((3, sl), F32)], axis=0)
    for k in order:
        send(st_m.at[a], st_m.at[a], ssem.at[11], rsem.at[11], along_a(k, c))
    await_bytes(st_m.at[pl.ds(0, n - 1)], rsem.at[11])
    ring_dots = sum(st_m[i, 0:1] for i in range(n))
    center0 = ring_dots / ring_total
    st_b[b] = jnp.concatenate([ring_peak, ring_total, ring_dots, blank[:1]], axis=0)
    for k in order:
        send(st_b.at[b], st_b.at[b], ssem.at[12], rsem.at[12], along_b(k, c))
    phase("a_send")
    for i in range(2):

        def grade(j, carry, i=i):
            at = pl.ds(pl.multiple_of(j * tile, tile), tile)
            to = pl.ds(pl.multiple_of(i * ts + j * tile, tile), tile)
            dr[to, :] = (p[i, at, :] * to_ring * (wg[i, at, :] - center0)).astype(BF16)
            return carry

        lax.fori_loop(0, ts // tile, grade, 0)
    own = reduce_first(asnd, arcv, ssem.at[13], rsem.at[13])

    phase("b_sum")
    await_bytes(brcv, rsem.at[10])
    low = bsum[...]
    for i in range(n - 1):
        low = low + brcv[i].astype(F32)

    phase("stat_b")
    await_bytes(st_b.at[pl.ds(0, n - 1)], rsem.at[12])
    tops = [st_b[i, 0:1] for i in range(n)]
    top = functools.reduce(jnp.maximum, tops)
    scales = [jnp.exp(t - top) for t in tops]
    norm = sum(st_b[i, 1:2] * s for i, s in enumerate(scales))
    center = sum(st_b[i, 2:3] * s for i, s in enumerate(scales)) / norm
    ring_scale = jnp.exp(ring_peak - top) / norm
    dev_scale = jnp.exp(peak - top) / norm
    for i in range(2):

        def settle(j, carry, i=i):
            at = pl.ds(pl.multiple_of(j * tile, tile), tile)
            dispatch = p[i, at, :] * dev_scale
            u[i, at, 0:sl] = dispatch.astype(BF16)
            u[i, at, sl : 2 * sl] = (dispatch * (wg[i, at, :] - center)).astype(BF16)
            return carry

        lax.fori_loop(0, ts // tile, settle, 0)
    low = low * (center - center0)

    phase("a_wait")
    await_bytes(arcv, rsem.at[13])
    for i in range(n - 1):
        own = own + arcv[i].astype(F32)
    r[...] = ((own - low) * ring_scale).reshape(n, rows, sl)
    for k in order:
        send(r.at[lax.rem(b + k, n)], rrcv.at[k - 1], ssem.at[14], rsem.at[14], along_b(k, c))

    phase("phi_wait")
    await_bytes(ph.at[pl.ds(0, n - 1)], rsem.at[9])
    for i in range(n):
        for j in range(n):
            at = ph.at[i * other + j * c, j * other + i * c]
            phim[(i * n + j) * rows : (i * n + j + 1) * rows] = at[...].astype(F32).reshape(rows, sl)
    w[sl : 2 * sl, :] = phim[...].T.astype(BF16)
    phase("emit_other")
    grad_scale = float(ts * n * n * 2 // 16)

    def emit_other(j, carry):
        at = pl.ds(pl.multiple_of(j * tile, tile), tile)
        s = jnp.dot(u[1, at, :], w[...], preferred_element_type=F32)
        tgs[at, :] = s.astype(BF16)
        send(tgs.at[at], tgr.at[at], osem.at[0], osem.at[1 + j], partner)
        return carry

    lax.fori_loop(0, ts // tile, emit_other, 0)

    phase("r_wait")
    res = r[b]
    await_bytes(rrcv, rsem.at[14])
    for k in range(n - 1):
        res = res + rrcv[k]
    xs[...] = res.reshape(2, rows // 2, sl)
    spot = x * 2 + c
    for k in far_first(nx):
        send(xs.at[c], xbuf.at[spot], ssem.at[15], rsem.at[15], along_x(k, c))
        send(xs.at[other], xbuf.at[spot], ssem.at[16], rsem.at[15], along_x(k, other))
    send(xs.at[other], xbuf.at[spot], ssem.at[16], rsem.at[15], partner)
    xbuf[spot] = xs[c]

    phase("emit_own")

    def emit_own(j, carry):
        at = pl.ds(pl.multiple_of(j * tile, tile), tile)
        s = jnp.dot(u[0, at, :], w[...], preferred_element_type=F32)
        await_bytes(tgr.at[at], osem.at[1 + j])
        tgs_own = (grad_scale * (s + tgr[at, :].astype(F32))).astype(BF16)
        tok[0, at, :] = tgs_own
        pltpu.make_async_copy(tok.at[0, at], tg_o.at[at], lsem.at[0]).start()
        return carry

    lax.fori_loop(0, ts // tile, emit_own, 0)

    phase("x_wait")
    await_bytes(xbuf.at[pl.ds(0, 2 * nx - 1)], rsem.at[15])
    for h in range(2):
        res = xbuf[h]
        for i in range(1, nx):
            res = res + xbuf[2 * i + h]
        pg_o[:, h * sl : (h + 1) * sl] = res

    phase("drain")
    await_bytes(l1.at[pl.ds(0, n - 1), 0], ssem.at[0])
    await_bytes(l1.at[:, 0], ssem.at[1])
    await_bytes(logv.at[1], ssem.at[2])
    await_bytes(ph.at[0, pl.ds(0, n - 1), 0], ssem.at[3])
    await_bytes(ph.at[0, :, 0], ssem.at[4])
    await_bytes(tok.at[1], ssem.at[5])
    await_bytes(st_a.at[pl.ds(0, n - 1)], ssem.at[6])
    await_bytes(gh.at[:, :, pl.ds(0, n - 1)], ssem.at[7])

    @pl.when((c == 0) & (near == 1))
    def _():
        await_bytes(l1, ssem.at[8])

    @pl.when(c == 1)
    def _():
        await_bytes(l1.at[pl.ds(0, nh)], ssem.at[8])

    await_bytes(ph.at[pl.ds(0, n - 1)], ssem.at[9])
    await_bytes(brcv, ssem.at[10])
    await_bytes(st_m.at[pl.ds(0, n - 1)], ssem.at[11])
    await_bytes(st_b.at[pl.ds(0, n - 1)], ssem.at[12])
    await_bytes(arcv, ssem.at[13])
    await_bytes(rrcv, ssem.at[14])
    await_bytes(xbuf.at[pl.ds(0, nx - 1)], ssem.at[15])
    await_bytes(xbuf.at[pl.ds(0, nx)], ssem.at[16])
    await_bytes(tgs, osem.at[0])
    await_bytes(tok.at[0], lsem.at[0])
    open_scope.close()


def per_device(n, nx, tokens, logits, slot_grad, phi_param):
    tokens, logits, slot_grad = tokens[0], logits[0], slot_grad[0]
    ts, d = tokens.shape
    sl = logits.shape[1] // 2
    rows = d // (n * n)
    gs = slot_grad.shape[0]
    half = d // 2
    tile = min(256, ts)
    vm, dma = pltpu.VMEM, pltpu.SemaphoreType.DMA
    any_spec = pl.BlockSpec(memory_space=pl.ANY)
    scratch = [
        vm((2, ts, d), BF16), vm((d, 2 * ts), BF16), vm((2, ts, sl), BF16),
        vm((2, ts, sl), F32), vm((2, ts, sl), F32), vm((2 * ts, sl), BF16),
        vm((2, ts, 2 * sl), BF16), vm((2 * sl, d), BF16), vm((d, sl), F32),
        vm((gs, half), BF16), vm((rows // 2, sl), BF16),
        vm((n, 2, gs, half), BF16), vm((2, n // 2, n, 2, gs, half), BF16),
        vm((n, n, 2, rows // 2, sl), BF16),
        vm((n, 4, sl), F32), vm((n, 4, sl), F32), vm((n, 4, sl), F32),
        vm((n - 1, n * rows, sl), BF16), vm((n - 1, n * rows, sl), BF16),
        vm((n - 1, n * rows, sl), BF16), vm((n - 1, n * rows, sl), BF16),
        vm((n * rows, sl), F32), vm((n, rows, sl), F32), vm((n - 1, rows, sl), F32),
        vm((2, rows // 2, sl), F32), vm((2 * nx, rows // 2, sl), F32),
        vm((ts, d), BF16), vm((ts, d), BF16),
        dma((6,)), dma((17,)), dma((16,)), dma((1 + ts // tile,)),
    ]
    token_grad, phi_grad = pl.pallas_call(
        functools.partial(kernel, n, nx),
        out_shape=(
            jax.ShapeDtypeStruct((ts, d), BF16),
            jax.ShapeDtypeStruct((rows // 2, 2 * sl), F32),
        ),
        in_specs=[any_spec] * 4,
        out_specs=(any_spec, pl.BlockSpec(memory_space=pltpu.VMEM)),
        scratch_shapes=scratch,
        compiler_params=pltpu.CompilerParams(
            collective_id=0, has_side_effects=True, vmem_limit_bytes=67043328
        ),
        name="moe_dispatch_backward",
    )(tokens, logits, slot_grad, phi_param)
    return token_grad[None], phi_grad


def solution(mesh):
    count, nx = mesh.devices.shape
    n = 8 if count == 128 else 2
    finer = Mesh(mesh.devices.reshape(n, n, 2, nx), (*SEQ, "batch"))
    in_specs = (P("batch", SEQ, None), P("batch", SEQ, None), P("batch", SEQ, None), P(SEQ, None))
    out_specs = (P("batch", SEQ, None), P(SEQ, None))
    return jax.shard_map(
        functools.partial(per_device, n, nx),
        mesh=finer, in_specs=in_specs, out_specs=out_specs, check_vma=False,
    )
```

```python
import contextlib
import functools

import jax
import jax.numpy as jnp
from jax import lax
from jax.experimental import pallas as pl
from jax.experimental.pallas import tpu as pltpu
from jax.sharding import Mesh
from jax.sharding import PartitionSpec as P

SEQ = ("seq_0", "seq_1", "seq_2")
MESH = pl.DeviceIdType.MESH
F32 = jnp.float32
BF16 = jnp.bfloat16
NT = (((1,), (1,)), ((), ()))


def far_first(n):
    return sorted(range(1, n), key=lambda k: (-min(k, n - k), k))


def kernel(
    n, nx, tok_h, log_h, g_h, phi_h, tg_o, pg_o,
    tok, tokT, logv, p, wg, dr, u, w, phim,
    g_other, p_other, l1, gh, ph, st_a, st_m, st_b, fin_out, fin,
    asnd, arcv, bsnd, brcv, mine_b, bhl, r, rrcv, xs, xbuf, tgs, tgr,
    lsem, ssem, rsem, gsem, osem,
):
    open_scope = contextlib.ExitStack()

    def phase(name):
        open_scope.close()
        open_scope.enter_context(jax.named_scope(name))

    phase("greet")
    z, y, c, x = (lax.axis_index(a) for a in (*SEQ, "batch"))
    other = 1 - c
    a = z * other + y * c
    b = y * other + z * c
    _, ts, d = tok.shape
    sl = logv.shape[2]
    half = d // 2
    rows = d // (n * n)
    tile = min(256, ts)
    order = far_first(n)

    def along_a(k, core):
        return (lax.rem(z + k * other, n), lax.rem(y + k * c, n), core, x)

    def along_b(k, core):
        return (lax.rem(z + k * c, n), lax.rem(y + k * other, n), core, x)

    def along_x(k, core):
        return (z, y, core, lax.rem(x + k, nx))

    partner = (z, y, other, x)

    def send(src, dst, s, q, to):
        pltpu.make_async_remote_copy(
            src_ref=src, dst_ref=dst, send_sem=s, recv_sem=q, device_id=to, device_id_type=MESH
        ).start()

    def await_bytes(ref, sem):
        pltpu.make_async_copy(ref, ref, sem).wait()

    mine = pl.ds(pl.multiple_of(c * half, half), half)
    theirs = pl.ds(pl.multiple_of(other * half, half), half)
    my_slots = pl.ds(pl.multiple_of(c * sl, sl), sl)
    their_slots = pl.ds(pl.multiple_of(other * sl, sl), sl)
    loads = [
        pltpu.make_async_copy(g_h.at[:, mine], l1.at[b, c], lsem.at[0]),
        pltpu.make_async_copy(g_h.at[:, theirs], g_other, lsem.at[1]),
        pltpu.make_async_copy(phi_h.at[:, my_slots], ph.at[a, b, c], lsem.at[2]),
        pltpu.make_async_copy(phi_h.at[:, their_slots], p_other, lsem.at[3]),
        pltpu.make_async_copy(log_h.at[:, my_slots], logv.at[0], lsem.at[4]),
        pltpu.make_async_copy(tok_h, tok.at[0], lsem.at[5]),
    ]
    loads[0].start()
    loads[1].start()

    barrier = pltpu.get_barrier_semaphore()
    peers = [partner]
    for k in order:
        for core in (c, other):
            peers += [along_a(k, core), along_b(k, core)]
    for k in range(1, nx):
        peers += [along_x(k, core) for core in (c, other)]
    for to in peers:
        pl.semaphore_signal(barrier, inc=1, device_id=to, device_id_type=MESH)
    for one in loads[2:]:
        one.start()
    loads[0].wait()
    loads[1].wait()
    pl.semaphore_wait(barrier, len(peers))

    def along_z(k, core):
        return (lax.rem(z + k, n), y, core, x)

    def along_y(k, core):
        return (z, lax.rem(y + k, n), core, x)

    phase("g1_send")
    for k in order:
        send(l1.at[b, c], l1.at[b, c], ssem.at[0], rsem.at[0], along_b(k, c))
        send(g_other, l1.at[a, c], ssem.at[1], rsem.at[1], along_a(k, other))
    send(g_other, l1.at[a, c], ssem.at[1], rsem.at[1], partner)
    send(log_h.at[:, their_slots], logv.at[1], ssem.at[2], rsem.at[2], partner)
    loads[2].wait()
    loads[3].wait()
    for k in order:
        send(ph.at[a, b, c], ph.at[a, b, c], ssem.at[3], rsem.at[3], along_b(k, c))
        send(p_other, ph.at[b, a, c], ssem.at[4], rsem.at[4], along_a(k, other))
    send(p_other, ph.at[b, a, c], ssem.at[4], rsem.at[4], partner)
    send(tok_h, tok.at[1], ssem.at[5], rsem.at[5], partner)

    phase("peak")
    loads[4].wait()
    await_bytes(logv.at[1], rsem.at[2])
    peak = jnp.max(logv[...].astype(F32), axis=(0, 1))[None]
    total = jnp.zeros((1, sl), F32)
    for i in range(2):
        raw = jnp.exp(logv[i].astype(F32) - peak)
        p[i] = raw
        total = total + jnp.sum(raw, axis=0, keepdims=True)
    blank = jnp.zeros((2, sl), F32)
    st_a[a] = jnp.concatenate([peak, total, blank], axis=0)
    for k in order:
        send(st_a.at[a], st_a.at[a], ssem.at[6], rsem.at[6], along_a(k, c))

    lanes = n * rows

    def turn(i):
        for j in range(n):
            blk = tok[i, :, j * lanes : (j + 1) * lanes].T
            for m in range(n):
                ja = j * other + m * c
                jb = m * other + j * c
                row = (lax.rem(ja - a + 2 * n - 1, n) * n + jb) * rows
                tokT[pl.ds(pl.multiple_of(row, rows), rows), i * ts : (i + 1) * ts] = blk[
                    m * rows : (m + 1) * rows
                ]

    phase("turn0")
    loads[5].wait()
    turn(0)

    phase("g1_wait")
    await_bytes(l1.at[pl.ds(0, n - 1), 0], rsem.at[0])
    await_bytes(l1.at[:, 0], rsem.at[1])
    nh = n // 2
    near = lax.div(z, nh)
    zz = lax.rem(z, nh)

    @pl.when(c == 0)
    def _():
        for k in order:
            send(l1, gh.at[0, zz], ssem.at[7], gsem.at[zz], along_a(k, near))

        @pl.when(near == 0)
        def _():
            pltpu.make_async_copy(l1, gh.at[0, zz], gsem.at[zz]).start()

        @pl.when(near == 1)
        def _():
            send(l1, gh.at[0, zz], ssem.at[8], gsem.at[zz], partner)

    @pl.when(c == 1)
    def _():
        for k in order:
            for q in range(2):
                send(
                    l1.at[pl.ds(q * nh, nh)], gh.at[1, :, y], ssem.at[7], rsem.at[8],
                    along_a(k, q),
                )
        send(l1.at[pl.ds(0, nh)], gh.at[1, :, y], ssem.at[8], rsem.at[8], partner)
        pltpu.make_async_copy(l1.at[pl.ds(nh, nh)], gh.at[1, :, y], rsem.at[8]).start()

    phase("phi_send")
    await_bytes(ph.at[0, pl.ds(0, n - 1), 0], rsem.at[3])
    await_bytes(ph.at[0, :, 0], rsem.at[4])
    for k in order:
        send(ph.at[a], ph.at[a], ssem.at[9], rsem.at[9], along_a(k, c))

    phase("turn1")
    await_bytes(tok.at[1], rsem.at[5])
    turn(1)

    phase("ml_wait")
    await_bytes(st_a.at[pl.ds(0, n - 1)], rsem.at[6])
    tops = [st_a[i, 0:1] for i in range(n)]
    ring_peak = functools.reduce(jnp.maximum, tops)
    ring_total = sum(st_a[i, 1:2] * jnp.exp(t - ring_peak) for i, t in enumerate(tops))
    to_ring = jnp.exp(peak - ring_peak)

    mass = jnp.zeros((1, sl), F32)
    for i in range(2):
        low = (p[i] * to_ring).astype(BF16)
        dr[i * ts : (i + 1) * ts] = low
        mass = mass + jnp.sum(low.astype(F32), axis=0, keepdims=True)

    blk = n * rows

    def chip_sums(visit):
        for start in sorted(range(0, n, 2), key=lambda i: -max(min(i + 1, n - i - 1), min(i + 2, n - i - 2))):
            res = jnp.dot(
                tokT[start * blk : (start + 2) * blk], dr[...], preferred_element_type=F32
            )
            for i in sorted(range(start, start + 2), key=lambda i: -min(i + 1, n - i - 1)):
                visit(i, res[(i - start) * blk : (i - start + 1) * blk])

    def hand_on(i, snd, rcv, s, t, q):
        if i < n - 1:
            send(snd.at[i], rcv.at[c, i], ssem.at[s], rsem.at[q + c], along_a(i + 1, 1))
            return

        @pl.when(c == 0)
        def _():
            send(snd.at[i], rcv.at[0, i], ssem.at[t], rsem.at[q], partner)

        @pl.when(c == 1)
        def _():
            pltpu.make_async_copy(snd.at[i], rcv.at[1, i], rsem.at[q + 1]).start()

    def b_visit(i, part):
        high = part.astype(BF16)
        bsnd[i] = high
        hand_on(i, bsnd, brcv, 10, 22, 10)
        rest = (part - high.astype(F32)).astype(BF16)
        ja = lax.rem(a + i + 1, n)
        for jb in range(n):
            row = ((ja * other + jb * c) * n + jb * other + ja * c) * rows
            at = pl.ds(pl.multiple_of(row, rows), rows)
            bhl[at, 0:sl] = high[jb * rows : (jb + 1) * rows]
            bhl[at, sl : 2 * sl] = rest[jb * rows : (jb + 1) * rows]

    def a_visit(i, part):
        asnd[i] = part.astype(BF16)
        hand_on(i, asnd, arcv, 13, 14, 12)

    phase("b_send")
    chip_sums(b_visit)

    per = n * 2 * gh.shape[4]

    def gather_rows(h, i):
        parts = [gh[h, i, j, k].astype(F32) for j in range(n) for k in range(2)]
        w[i * per : (i + 1) * per, h * half : (h + 1) * half] = jnp.concatenate(
            parts, axis=0
        ).astype(BF16)

    phase("g2_wait")
    for i in range(nh):
        await_bytes(gh.at[0, i], gsem.at[i])
        gather_rows(0, i)
    await_bytes(gh.at[1], rsem.at[8])
    phase("dots")
    for i in range(nh):
        gather_rows(1, i)
    prod = jnp.dot(w[0:sl, :], bhl[...], preferred_element_type=F32)
    at_row = lax.broadcasted_iota(jnp.int32, (sl, 2 * sl), 0)
    at_col = lax.broadcasted_iota(jnp.int32, (sl, 2 * sl), 1)
    prod = jnp.where((at_row == at_col) | (at_row + sl == at_col), prod, 0.0)
    prod = jnp.sum(prod, axis=0, keepdims=True)
    dots = prod[:, 0:sl] + prod[:, sl : 2 * sl]
    st_m[c, a] = jnp.concatenate([dots, mass, ring_peak, ring_total], axis=0)
    for k in order:
        send(st_m.at[c, a], st_m.at[c, a], ssem.at[11], rsem.at[14 + c], along_a(k, 1))

    @pl.when(c == 0)
    def _():
        send(st_m.at[c, a], st_m.at[c, a], ssem.at[12], rsem.at[14], partner)

    def mean_of(total, weight):
        some = weight > 0.0
        return jnp.where(some, total / jnp.where(some, weight, 1.0), 0.0)

    center_dev = mean_of(dots, mass)

    phase("weigh")
    for i in range(2):
        for j in range(ts // tile):
            at = pl.ds(j * tile, tile)
            v = lax.dot_general(tok[i, at, :], w[0:sl, :], NT, preferred_element_type=F32)
            wg[i, at, :] = v
            dr[pl.ds(i * ts + j * tile, tile), :] = (
                p[i, at, :] * to_ring * (v - center_dev)
            ).astype(BF16)
    phase("a_send")
    chip_sums(a_visit)

    phase("b_wait")
    at_b = (y, z)
    to_b = (along_y, along_z)

    def spread(h, q, value):
        r[q, h] = value.reshape(n, rows, sl)
        for k in order:
            send(
                r.at[q, h, lax.rem(at_b[h] + k, n)], rrcv.at[q, h, at_b[h]], ssem.at[21],
                rsem.at[17 + q], to_b[h](k, 1),
            )
        rrcv[q, h, at_b[h]] = r[q, h, at_b[h]]

    @pl.when(c == 1)
    def _():
        await_bytes(brcv.at[0], rsem.at[10])
        await_bytes(brcv.at[1], rsem.at[11])
        for h in range(2):
            spread(h, 0, sum(brcv[h, i].astype(F32) for i in range(n)))
        phase("m_wait")
        await_bytes(st_m.at[0], rsem.at[14])
        await_bytes(st_m.at[1, pl.ds(0, n - 1)], rsem.at[15])
        ring_at = (z, y)
        for h in range(2):
            sums = [sum(st_m[h, i, q : q + 1] for i in range(n)) for q in range(2)]
            st_b[h, at_b[h]] = jnp.concatenate([*sums, st_m[h, 0, 2:4]], axis=0)
            for k in order:
                spot = st_b.at[h, at_b[h]]
                send(spot, spot, ssem.at[19], rsem.at[16], to_b[h](k, 1))
        for h in range(2):
            low = jnp.zeros((blk, sl), F32)
            for i in range(n):
                peer = lax.rem(ring_at[h] + 2 * n - 1 - i, n)
                low = low + mean_of(st_m[h, peer, 0:1], st_m[h, peer, 1:2]) * brcv[h, i].astype(F32)
            mine_b[h] = low
        phase("a_wait")
        await_bytes(arcv.at[0], rsem.at[12])
        await_bytes(arcv.at[1], rsem.at[13])
        for h in range(2):
            res = mine_b[h]
            for i in range(n):
                res = res + arcv[h, i].astype(F32)
            spread(h, 1, res)
        phase("centers")
        await_bytes(st_b.at[:, pl.ds(0, n - 1)], rsem.at[16])
        for h in range(2):
            tops = [st_b[h, i, 2:3] for i in range(n)]
            top = functools.reduce(jnp.maximum, tops)
            scales = [jnp.exp(t - top) for t in tops]
            dot_sum, weight, norm = (
                sum(st_b[h, i, q : q + 1] * s for i, s in enumerate(scales)) for q in (0, 1, 3)
            )
            fin_out[h] = jnp.concatenate([dot_sum / weight, top, norm, blank[:1]], axis=0)
        send(fin_out.at[0], fin, ssem.at[20], rsem.at[19], partner)
        fin[...] = fin_out[1]

    @pl.when(c == 0)
    def _():
        await_bytes(fin, rsem.at[19])

    phase("settle")
    center = fin[0:1]
    dev_scale = jnp.exp(peak - fin[1:2]) / fin[2:3]
    for i in range(2):

        def settle(j, carry, i=i):
            at = pl.ds(pl.multiple_of(j * tile, tile), tile)
            dispatch = p[i, at, :] * dev_scale
            u[i, at, 0:sl] = dispatch.astype(BF16)
            u[i, at, sl : 2 * sl] = (dispatch * (wg[i, at, :] - center)).astype(BF16)
            return carry

        lax.fori_loop(0, ts // tile, settle, 0)

    phase("phi_wait")
    await_bytes(ph.at[pl.ds(0, n - 1)], rsem.at[9])
    for i in range(n):
        for j in range(n):
            at = ph.at[i * other + j * c, j * other + i * c]
            phim[(i * n + j) * rows : (i * n + j + 1) * rows] = at[...].astype(F32).reshape(rows, sl)
    w[sl : 2 * sl, :] = phim[...].T.astype(BF16)
    phase("emit_other")
    grad_scale = float(ts * n * n * 2 // 16)

    def emit_other(j, carry):
        at = pl.ds(pl.multiple_of(j * tile, tile), tile)
        s = jnp.dot(u[1, at, :], w[...], preferred_element_type=F32)
        tgs[at, :] = s.astype(BF16)
        send(tgs.at[at], tgr.at[at], osem.at[0], osem.at[1 + j], partner)
        return carry

    lax.fori_loop(0, ts // tile, emit_other, 0)

    phase("r_wait")

    @pl.when(c == 1)
    def _():
        await_bytes(rrcv.at[0, :, pl.ds(0, n - 1)], rsem.at[17])
        await_bytes(rrcv.at[1, :, pl.ds(0, n - 1)], rsem.at[18])
        for h in range(2):
            res = jnp.zeros((rows, sl), F32)
            for i in range(n):
                ring_scale = jnp.exp(st_b[h, i, 2:3] - fin_out[h, 1:2]) / fin_out[h, 2:3]
                res = res + (rrcv[1, h, i] - fin_out[h, 0:1] * rrcv[0, h, i]) * ring_scale
            xs[:, :, h * sl : (h + 1) * sl] = res.reshape(2, rows // 2, sl)
        for k in far_first(nx):
            for core in range(2):
                send(xs.at[core], xbuf.at[x], ssem.at[15], rsem.at[20], along_x(k, core))
        send(xs.at[0], xbuf.at[x], ssem.at[16], rsem.at[20], partner)
        xbuf[x] = xs[1]

    phase("emit_own")

    def emit_own(j, carry):
        at = pl.ds(pl.multiple_of(j * tile, tile), tile)
        s = jnp.dot(u[0, at, :], w[...], preferred_element_type=F32)
        await_bytes(tgr.at[at], osem.at[1 + j])
        tg_o[at, :] = (grad_scale * (s + tgr[at, :].astype(F32))).astype(BF16)
        return carry

    lax.fori_loop(0, ts // tile, emit_own, 0)

    phase("x_wait")
    @pl.when(c == 0)
    def _():
        await_bytes(xbuf, rsem.at[20])

    @pl.when(c == 1)
    def _():
        await_bytes(xbuf.at[pl.ds(0, nx - 1)], rsem.at[20])

    res = xbuf[0]
    for i in range(1, nx):
        res = res + xbuf[i]
    pg_o[...] = res

    phase("drain")
    await_bytes(l1.at[pl.ds(0, n - 1), 0], ssem.at[0])
    await_bytes(l1.at[:, 0], ssem.at[1])
    await_bytes(gh.at[:, :, pl.ds(0, n - 1)], ssem.at[7])
    await_bytes(logv.at[1], ssem.at[2])
    await_bytes(ph.at[0, pl.ds(0, n - 1), 0], ssem.at[3])
    await_bytes(ph.at[0, :, 0], ssem.at[4])
    await_bytes(tok.at[1], ssem.at[5])
    await_bytes(st_a.at[pl.ds(0, n - 1)], ssem.at[6])
    await_bytes(ph.at[pl.ds(0, n - 1)], ssem.at[9])
    await_bytes(brcv.at[0, pl.ds(0, n - 1)], ssem.at[10])
    await_bytes(st_m.at[0, pl.ds(0, n - 1)], ssem.at[11])
    await_bytes(arcv.at[0, pl.ds(0, n - 1)], ssem.at[13])
    await_bytes(tgs, osem.at[0])

    @pl.when((c == 0) & (near == 1))
    def _():
        await_bytes(l1, ssem.at[8])

    @pl.when(c == 0)
    def _():
        await_bytes(brcv.at[0, 0], ssem.at[22])
        await_bytes(arcv.at[0, 0], ssem.at[14])
        await_bytes(st_m.at[0, 0], ssem.at[12])

    @pl.when(c == 1)
    def _():
        await_bytes(l1.at[pl.ds(0, nh)], ssem.at[8])
        await_bytes(st_b.at[:, pl.ds(0, n - 1)], ssem.at[19])
        await_bytes(fin, ssem.at[20])
        await_bytes(rrcv.at[:, :, pl.ds(0, n - 1)], ssem.at[21])
        await_bytes(xbuf.at[pl.ds(0, nx - 1)], ssem.at[15])
        await_bytes(xbuf.at[pl.ds(0, nx - 1)], ssem.at[15])
        await_bytes(xbuf.at[0], ssem.at[16])

    open_scope.close()


def write_out(tg_v, pg_v, tg_o, pg_o, sem):
    parts = 8
    copies = [pltpu.make_async_copy(pg_v, pg_o, sem.at[parts])]
    size = tg_v.shape[0] // parts
    for i in range(parts):
        at = pl.ds(i * size, size)
        copies.append(pltpu.make_async_copy(tg_v.at[at], tg_o.at[at], sem.at[i]))
    for one in copies:
        one.start()
    for one in copies:
        one.wait()


def per_device(n, nx, tokens, logits, slot_grad, phi_param):
    tokens, logits, slot_grad = tokens[0], logits[0], slot_grad[0]
    ts, d = tokens.shape
    sl = logits.shape[1] // 2
    rows = d // (n * n)
    gs = slot_grad.shape[0]
    half = d // 2
    tile = min(256, ts)
    vm, dma = pltpu.VMEM, pltpu.SemaphoreType.DMA
    any_spec = pl.BlockSpec(memory_space=pl.ANY)
    scratch = [
        vm((2, ts, d), BF16), vm((d, 2 * ts), BF16), vm((2, ts, sl), BF16),
        vm((2, ts, sl), F32), vm((2, ts, sl), F32), vm((2 * ts, sl), BF16),
        vm((2, ts, 2 * sl), BF16), vm((2 * sl, d), BF16), vm((d, sl), F32),
        vm((gs, half), BF16), vm((rows // 2, sl), BF16),
        vm((n, 2, gs, half), BF16), vm((2, n // 2, n, 2, gs, half), BF16),
        vm((n, n, 2, rows // 2, sl), BF16),
        vm((n, 4, sl), F32), vm((2, n, 4, sl), F32), vm((2, n, 4, sl), F32),
        vm((2, 4, sl), F32), vm((4, sl), F32),
        vm((n, n * rows, sl), BF16), vm((2, n, n * rows, sl), BF16),
        vm((n, n * rows, sl), BF16), vm((2, n, n * rows, sl), BF16),
        vm((2, n * rows, sl), F32), vm((d, 2 * sl), BF16),
        vm((2, 2, n, rows, sl), F32), vm((2, 2, n, rows, sl), F32),
        vm((2, rows // 2, 2 * sl), F32), vm((nx, rows // 2, 2 * sl), F32),
        vm((ts, d), BF16), vm((ts, d), BF16),
        dma((6,)), dma((23,)), dma((21,)), dma((n // 2,)), dma((1 + ts // tile,)),
    ]
    vm_spec = pl.BlockSpec(memory_space=pltpu.VMEM)
    token_grad, phi_grad = pl.pallas_call(
        functools.partial(kernel, n, nx),
        out_shape=(pltpu.VMEM((ts, d), BF16), pltpu.VMEM((rows // 2, 2 * sl), F32)),
        in_specs=[any_spec] * 4,
        out_specs=(vm_spec, vm_spec),
        scratch_shapes=scratch,
        compiler_params=pltpu.CompilerParams(
            collective_id=0, has_side_effects=True, vmem_limit_bytes=56000000
        ),
        name="moe_dispatch_backward",
    )(tokens, logits, slot_grad, phi_param)
    token_grad, phi_grad = pl.pallas_call(
        write_out,
        out_shape=(
            jax.ShapeDtypeStruct((ts, d), BF16),
            jax.ShapeDtypeStruct((rows // 2, 2 * sl), F32),
        ),
        in_specs=[any_spec, any_spec],
        out_specs=(any_spec, any_spec),
        scratch_shapes=[dma((9,))],
        compiler_params=pltpu.CompilerParams(vmem_limit_bytes=4 * 1024 * 1024),
        name="write_out",
    )(token_grad, phi_grad)
    return token_grad[None], phi_grad


def solution(mesh):
    count, nx = mesh.devices.shape
    n = round((count // 2) ** 0.5)
    finer = Mesh(mesh.devices.reshape(n, n, 2, nx), (*SEQ, "batch"))
    in_specs = (P("batch", SEQ, None), P("batch", SEQ, None), P("batch", SEQ, None), P(SEQ, None))
    out_specs = (P("batch", SEQ, None), P(SEQ, None))
    return jax.shard_map(
        functools.partial(per_device, n, nx),
        mesh=finer, in_specs=in_specs, out_specs=out_specs, check_vma=False,
    )
```

```python
import contextlib
import functools

import jax
import jax.numpy as jnp
from jax import lax
from jax.experimental import pallas as pl
from jax.experimental.pallas import tpu as pltpu
from jax.sharding import Mesh
from jax.sharding import PartitionSpec as P

SEQ = ("seq_0", "seq_1", "seq_2")
MESH = pl.DeviceIdType.MESH
F32 = jnp.float32
BF16 = jnp.bfloat16
NT = (((1,), (1,)), ((), ()))


def far_first(n):
    return sorted(range(1, n), key=lambda k: (-min(k, n - k), k))


def kernel(
    n, nx, tok_h, log_h, g_h, phi_h, tg_o, pg_o,
    tok, tokT, logv, p, wg, dr, u, w, phim,
    g_other, p_other, l1, gh, ph, st_a, st_m, st_b, fin_out, fin,
    asnd, arcv, bsnd, brcv, mine_b, bhl, r, rrcv, xs, xbuf, po, wo, pko,
    lsem, ssem, rsem, gsem,
):
    open_scope = contextlib.ExitStack()

    def phase(name):
        open_scope.close()
        open_scope.enter_context(jax.named_scope(name))

    phase("greet")
    z, y, c, x = (lax.axis_index(a) for a in (*SEQ, "batch"))
    other = 1 - c
    a = z * other + y * c
    b = y * other + z * c
    _, ts, d = tok.shape
    sl = logv.shape[2]
    half = d // 2
    rows = d // (n * n)
    tile = min(256, ts)
    order = far_first(n)

    def along_a(k, core):
        return (lax.rem(z + k * other, n), lax.rem(y + k * c, n), core, x)

    def along_b(k, core):
        return (lax.rem(z + k * c, n), lax.rem(y + k * other, n), core, x)

    def along_x(k, core):
        return (z, y, core, lax.rem(x + k, nx))

    partner = (z, y, other, x)

    def send(src, dst, s, q, to):
        pltpu.make_async_remote_copy(
            src_ref=src, dst_ref=dst, send_sem=s, recv_sem=q, device_id=to, device_id_type=MESH
        ).start()

    def await_bytes(ref, sem):
        pltpu.make_async_copy(ref, ref, sem).wait()

    mine = pl.ds(pl.multiple_of(c * half, half), half)
    theirs = pl.ds(pl.multiple_of(other * half, half), half)
    my_slots = pl.ds(pl.multiple_of(c * sl, sl), sl)
    their_slots = pl.ds(pl.multiple_of(other * sl, sl), sl)
    loads = [
        pltpu.make_async_copy(g_h.at[:, mine], l1.at[b, c], lsem.at[0]),
        pltpu.make_async_copy(g_h.at[:, theirs], g_other, lsem.at[1]),
        pltpu.make_async_copy(phi_h.at[:, my_slots], ph.at[0, b, c], lsem.at[2]),
        pltpu.make_async_copy(phi_h.at[:, their_slots], p_other, lsem.at[3]),
        pltpu.make_async_copy(log_h.at[:, my_slots], logv.at[0], lsem.at[4]),
        pltpu.make_async_copy(tok_h, tok.at[0], lsem.at[5]),
    ]
    loads[0].start()
    loads[1].start()

    barrier = pltpu.get_barrier_semaphore()
    peers = [partner]
    for k in order:
        for core in (c, other):
            peers += [along_a(k, core), along_b(k, core)]
    for k in range(1, nx):
        peers += [along_x(k, core) for core in (c, other)]
    for to in peers:
        pl.semaphore_signal(barrier, inc=1, device_id=to, device_id_type=MESH)
    for one in loads[2:]:
        one.start()
    loads[0].wait()
    loads[1].wait()
    pl.semaphore_wait(barrier, len(peers))

    def along_z(k, core):
        return (lax.rem(z + k, n), y, core, x)

    def along_y(k, core):
        return (z, lax.rem(y + k, n), core, x)

    phase("g1_send")
    for k in order:
        send(l1.at[b, c], l1.at[b, c], ssem.at[0], rsem.at[0], along_b(k, c))
        send(g_other, l1.at[a, c], ssem.at[1], rsem.at[1], along_a(k, other))
    send(g_other, l1.at[a, c], ssem.at[1], rsem.at[1], partner)
    send(log_h.at[:, their_slots], logv.at[1], ssem.at[2], rsem.at[2], partner)
    loads[2].wait()
    loads[3].wait()
    for k in order:
        send(ph.at[0, b, c], ph.at[0, b, c], ssem.at[3], rsem.at[3], along_b(k, c))
        send(p_other, ph.at[0, a, c], ssem.at[4], rsem.at[4], along_a(k, other))
    send(p_other, ph.at[0, a, c], ssem.at[4], rsem.at[4], partner)
    send(tok_h, tok.at[1], ssem.at[5], rsem.at[5], partner)

    phase("peak")
    loads[4].wait()
    await_bytes(logv.at[1], rsem.at[2])
    peak = jnp.max(logv[...].astype(F32), axis=(0, 1))[None]
    total = jnp.zeros((1, sl), F32)
    for i in range(2):
        raw = jnp.exp(logv[i].astype(F32) - peak)
        p[i] = raw
        total = total + jnp.sum(raw, axis=0, keepdims=True)
    blank = jnp.zeros((2, sl), F32)
    st_a[a] = jnp.concatenate([peak, total, blank], axis=0)
    for k in order:
        send(st_a.at[a], st_a.at[a], ssem.at[6], rsem.at[6], along_a(k, c))

    lanes = n * rows

    def turn(i):
        for j in range(n):
            blk = tok[i, :, j * lanes : (j + 1) * lanes].T
            for m in range(n):
                ja = j * other + m * c
                jb = m * other + j * c
                row = (lax.rem(ja - a + 2 * n - 1, n) * n + jb) * rows
                tokT[pl.ds(pl.multiple_of(row, rows), rows), i * ts : (i + 1) * ts] = blk[
                    m * rows : (m + 1) * rows
                ]

    phase("turn0")
    loads[5].wait()
    turn(0)

    phase("g1_wait")
    await_bytes(l1.at[pl.ds(0, n - 1), 0], rsem.at[0])
    await_bytes(l1.at[:, 0], rsem.at[1])
    nh = n // 2
    near = lax.div(z, nh)
    zz = lax.rem(z, nh)

    @pl.when(c == 0)
    def _():
        for k in order:
            send(l1, gh.at[0, zz], ssem.at[7], gsem.at[zz], along_a(k, near))

        @pl.when(near == 0)
        def _():
            pltpu.make_async_copy(l1, gh.at[0, zz], gsem.at[zz]).start()

        @pl.when(near == 1)
        def _():
            send(l1, gh.at[0, zz], ssem.at[8], gsem.at[zz], partner)

    @pl.when(c == 1)
    def _():
        for k in order:
            for q in range(2):
                send(
                    l1.at[pl.ds(q * nh, nh)], gh.at[1, :, y], ssem.at[7], rsem.at[8],
                    along_a(k, q),
                )
        send(l1.at[pl.ds(0, nh)], gh.at[1, :, y], ssem.at[8], rsem.at[8], partner)
        pltpu.make_async_copy(l1.at[pl.ds(nh, nh)], gh.at[1, :, y], rsem.at[8]).start()

    phase("phi_send")
    await_bytes(ph.at[0, pl.ds(0, n - 1), 0], rsem.at[3])
    await_bytes(ph.at[0, :, 0], rsem.at[4])
    part = pl.ds(x * (n // nx), n // nx)
    for k in order:
        send(ph.at[0, part], ph.at[n - k, part], ssem.at[9], rsem.at[9], along_a(k, c))

    phase("turn1")
    await_bytes(tok.at[1], rsem.at[5])
    turn(1)

    phase("ml_wait")
    await_bytes(st_a.at[pl.ds(0, n - 1)], rsem.at[6])
    tops = [st_a[i, 0:1] for i in range(n)]
    ring_peak = functools.reduce(jnp.maximum, tops)
    ring_total = sum(st_a[i, 1:2] * jnp.exp(t - ring_peak) for i, t in enumerate(tops))
    to_ring = jnp.exp(peak - ring_peak)

    mass = jnp.zeros((1, sl), F32)
    for i in range(2):
        low = (p[i] * to_ring).astype(BF16)
        dr[i * ts : (i + 1) * ts] = low
        mass = mass + jnp.sum(low.astype(F32), axis=0, keepdims=True)

    blk = n * rows

    def chip_sums(visit):
        for start in sorted(range(0, n, 2), key=lambda i: -max(min(i + 1, n - i - 1), min(i + 2, n - i - 2))):
            res = jnp.dot(
                tokT[start * blk : (start + 2) * blk], dr[...], preferred_element_type=F32
            )
            for i in sorted(range(start, start + 2), key=lambda i: -min(i + 1, n - i - 1)):
                visit(i, res[(i - start) * blk : (i - start + 1) * blk])

    def hand_on(i, snd, rcv, s, t, q):
        if i < n - 1:
            send(snd.at[i], rcv.at[c, i], ssem.at[s], rsem.at[q + c], along_a(i + 1, 1))
            return

        @pl.when(c == 0)
        def _():
            send(snd.at[i], rcv.at[0, i], ssem.at[t], rsem.at[q], partner)

        @pl.when(c == 1)
        def _():
            pltpu.make_async_copy(snd.at[i], rcv.at[1, i], rsem.at[q + 1]).start()

    def b_visit(i, part):
        high = part.astype(BF16)
        bsnd[i] = high
        hand_on(i, bsnd, brcv, 10, 22, 10)
        rest = (part - high.astype(F32)).astype(BF16)
        ja = lax.rem(a + i + 1, n)
        for jb in range(n):
            row = ((ja * other + jb * c) * n + jb * other + ja * c) * rows
            at = pl.ds(pl.multiple_of(row, rows), rows)
            bhl[at, 0:sl] = high[jb * rows : (jb + 1) * rows]
            bhl[at, sl : 2 * sl] = rest[jb * rows : (jb + 1) * rows]

    def a_visit(i, part):
        asnd[i] = part.astype(BF16)
        hand_on(i, asnd, arcv, 13, 14, 12)

    phase("b_send")
    chip_sums(b_visit)

    per = n * 2 * gh.shape[4]

    def gather_rows(h, i):
        parts = [gh[h, i, j, k].astype(F32) for j in range(n) for k in range(2)]
        w[i * per : (i + 1) * per, h * half : (h + 1) * half] = jnp.concatenate(
            parts, axis=0
        ).astype(BF16)

    phase("g2_wait")
    for i in range(nh):
        await_bytes(gh.at[0, i], gsem.at[i])
        gather_rows(0, i)
    await_bytes(gh.at[1], rsem.at[8])
    phase("dots")
    for i in range(nh):
        gather_rows(1, i)
    prod = jnp.dot(w[0:sl, :], bhl[...], preferred_element_type=F32)
    at_row = lax.broadcasted_iota(jnp.int32, (sl, 2 * sl), 0)
    at_col = lax.broadcasted_iota(jnp.int32, (sl, 2 * sl), 1)
    prod = jnp.where((at_row == at_col) | (at_row + sl == at_col), prod, 0.0)
    prod = jnp.sum(prod, axis=0, keepdims=True)
    dots = prod[:, 0:sl] + prod[:, sl : 2 * sl]
    st_m[c, a] = jnp.concatenate([dots, mass, ring_peak, ring_total], axis=0)
    for k in order:
        send(st_m.at[c, a], st_m.at[c, a], ssem.at[11], rsem.at[14 + c], along_a(k, 1))

    @pl.when(c == 0)
    def _():
        send(st_m.at[c, a], st_m.at[c, a], ssem.at[12], rsem.at[14], partner)

    def mean_of(total, weight):
        some = weight > 0.0
        return jnp.where(some, total / jnp.where(some, weight, 1.0), 0.0)

    center_dev = mean_of(dots, mass)

    phase("weigh")
    for i in range(2):
        for j in range(ts // tile):
            at = pl.ds(j * tile, tile)
            v = lax.dot_general(tok[i, at, :], w[0:sl, :], NT, preferred_element_type=F32)
            wg[i, at, :] = v
            dr[pl.ds(i * ts + j * tile, tile), :] = (
                p[i, at, :] * to_ring * (v - center_dev)
            ).astype(BF16)
    far = pl.ds(1, n - 1)
    await_bytes(ph.at[far, pl.ds(0, n // nx)], rsem.at[9])
    for k in far_first(nx):
        send(ph.at[far, part], ph.at[far, part], ssem.at[28], rsem.at[26], along_x(k, c))
    phase("a_send")
    chip_sums(a_visit)

    phase("pair_send")
    pko[0] = jnp.concatenate([peak, peak, blank], axis=0)
    send(pko.at[0], pko.at[1], ssem.at[23], rsem.at[21], partner)
    send(p.at[1], po, ssem.at[24], rsem.at[22], partner)
    send(wg.at[1], wo, ssem.at[25], rsem.at[23], partner)
    send(w.at[pl.ds(0, sl)], w.at[pl.ds(2 * sl, sl)], ssem.at[26], rsem.at[24], partner)

    def phi_rows():
        phase("phi_wait")
        await_bytes(ph.at[far, pl.ds(0, n - n // nx)], rsem.at[26])
        for i in range(n):
            for j in range(n):
                at = ph.at[lax.rem(i * other + j * c + n - a, n), j * other + i * c]
                phim[(i * n + j) * rows : (i * n + j + 1) * rows] = at[...].astype(F32).reshape(rows, sl)
        w[sl : 2 * sl, :] = phim[...].T.astype(BF16)
        send(
            w.at[pl.ds(sl, sl)], w.at[pl.ds(3 * sl, sl)], ssem.at[27], rsem.at[25], partner
        )

    phase("b_wait")
    at_b = (y, z)
    to_b = (along_y, along_z)

    def spread(h, q, value):
        r[q, h] = value.reshape(n, rows, sl)
        for k in order:
            send(
                r.at[q, h, lax.rem(at_b[h] + k, n)], rrcv.at[q, h, at_b[h]], ssem.at[21],
                rsem.at[17 + q], to_b[h](k, 1),
            )
        rrcv[q, h, at_b[h]] = r[q, h, at_b[h]]

    @pl.when(c == 1)
    def _():
        phase("m_wait")
        await_bytes(st_m.at[0], rsem.at[14])
        await_bytes(st_m.at[1, pl.ds(0, n - 1)], rsem.at[15])
        ring_at = (z, y)
        for h in range(2):
            sums = [sum(st_m[h, i, q : q + 1] for i in range(n)) for q in range(2)]
            st_b[h, at_b[h]] = jnp.concatenate([*sums, st_m[h, 0, 2:4]], axis=0)
            for k in order:
                spot = st_b.at[h, at_b[h]]
                send(spot, spot, ssem.at[19], rsem.at[16], to_b[h](k, 1))
        await_bytes(brcv.at[0], rsem.at[10])
        await_bytes(brcv.at[1], rsem.at[11])
        for h in range(2):
            spread(h, 0, sum(brcv[h, i].astype(F32) for i in range(n)))
        for h in range(2):
            low = jnp.zeros((blk, sl), F32)
            for i in range(n):
                peer = lax.rem(ring_at[h] + 2 * n - 1 - i, n)
                low = low + mean_of(st_m[h, peer, 0:1], st_m[h, peer, 1:2]) * brcv[h, i].astype(F32)
            mine_b[h] = low
        phase("a_wait")
        await_bytes(arcv.at[0], rsem.at[12])
        await_bytes(arcv.at[1], rsem.at[13])
        for h in range(2):
            res = mine_b[h]
            for i in range(n):
                res = res + arcv[h, i].astype(F32)
            spread(h, 1, res)
        phi_rows()
        phase("centers")
        await_bytes(st_b.at[:, pl.ds(0, n - 1)], rsem.at[16])
        for h in range(2):
            tops = [st_b[h, i, 2:3] for i in range(n)]
            top = functools.reduce(jnp.maximum, tops)
            scales = [jnp.exp(t - top) for t in tops]
            dot_sum, weight, norm = (
                sum(st_b[h, i, q : q + 1] * s for i, s in enumerate(scales)) for q in (0, 1, 3)
            )
            fin_out[h] = jnp.concatenate([dot_sum / weight, top, norm, blank[:1]], axis=0)
        send(fin_out, fin, ssem.at[20], rsem.at[19], partner)
        fin[...] = fin_out[...]

    @pl.when(c == 0)
    def _():
        phi_rows()
        phase("fin_wait")
        await_bytes(fin, rsem.at[19])

    phase("pair_wait")
    await_bytes(pko.at[1], rsem.at[21])
    await_bytes(po, rsem.at[22])
    await_bytes(wo, rsem.at[23])
    await_bytes(w.at[pl.ds(0, sl)], rsem.at[24])
    await_bytes(w.at[pl.ds(0, sl)], rsem.at[25])
    phase("emit")
    grad_scale = float(ts * n * n * 2 // 16)
    halves = []
    for q, core in enumerate((c, other)):
        last = fin[core]
        scale = jnp.exp(pko[q, 0:1] - last[1:2]) / last[2:3]
        halves.append((last[0:1], scale))
    for j in range(ts // tile):
        at = pl.ds(j * tile, tile)
        for q, (pv, wv) in enumerate(((p[0, at, :], wg[0, at, :]), (po[at, :], wo[at, :]))):
            center, scale = halves[q]
            dispatch = pv * scale
            u[at, 2 * q * sl : (2 * q + 1) * sl] = dispatch.astype(BF16)
            u[at, (2 * q + 1) * sl : (2 * q + 2) * sl] = (dispatch * (wv - center)).astype(BF16)
        s = jnp.dot(u[at, :], w[...], preferred_element_type=F32)
        tg_o[at, :] = (grad_scale * s).astype(BF16)

    phase("r_wait")

    @pl.when(c == 1)
    def _():
        await_bytes(rrcv.at[0, :, pl.ds(0, n - 1)], rsem.at[17])
        await_bytes(rrcv.at[1, :, pl.ds(0, n - 1)], rsem.at[18])
        for h in range(2):
            res = jnp.zeros((rows, sl), F32)
            for i in range(n):
                ring_scale = jnp.exp(st_b[h, i, 2:3] - fin_out[h, 1:2]) / fin_out[h, 2:3]
                res = res + (rrcv[1, h, i] - fin_out[h, 0:1] * rrcv[0, h, i]) * ring_scale
            xs[:, :, h * sl : (h + 1) * sl] = res.reshape(2, rows // 2, sl)
        for k in far_first(nx):
            for core in range(2):
                send(xs.at[core], xbuf.at[x], ssem.at[15], rsem.at[20], along_x(k, core))
        send(xs.at[0], xbuf.at[x], ssem.at[16], rsem.at[20], partner)
        xbuf[x] = xs[1]

    phase("x_wait")
    @pl.when(c == 0)
    def _():
        await_bytes(xbuf, rsem.at[20])

    @pl.when(c == 1)
    def _():
        await_bytes(xbuf.at[pl.ds(0, nx - 1)], rsem.at[20])

    res = xbuf[0]
    for i in range(1, nx):
        res = res + xbuf[i]
    pg_o[...] = res

    phase("drain")
    await_bytes(l1.at[pl.ds(0, n - 1), 0], ssem.at[0])
    await_bytes(l1.at[:, 0], ssem.at[1])
    await_bytes(gh.at[:, :, pl.ds(0, n - 1)], ssem.at[7])
    await_bytes(logv.at[1], ssem.at[2])
    await_bytes(ph.at[0, pl.ds(0, n - 1), 0], ssem.at[3])
    await_bytes(ph.at[0, :, 0], ssem.at[4])
    await_bytes(tok.at[1], ssem.at[5])
    await_bytes(st_a.at[pl.ds(0, n - 1)], ssem.at[6])
    await_bytes(ph.at[far, pl.ds(0, n // nx)], ssem.at[9])
    await_bytes(ph.at[far, pl.ds(0, n - n // nx)], ssem.at[28])
    await_bytes(brcv.at[0, pl.ds(0, n - 1)], ssem.at[10])
    await_bytes(st_m.at[0, pl.ds(0, n - 1)], ssem.at[11])
    await_bytes(arcv.at[0, pl.ds(0, n - 1)], ssem.at[13])
    await_bytes(pko.at[0], ssem.at[23])
    await_bytes(po, ssem.at[24])
    await_bytes(wo, ssem.at[25])
    await_bytes(w.at[pl.ds(0, sl)], ssem.at[26])
    await_bytes(w.at[pl.ds(0, sl)], ssem.at[27])

    @pl.when((c == 0) & (near == 1))
    def _():
        await_bytes(l1, ssem.at[8])

    @pl.when(c == 0)
    def _():
        await_bytes(brcv.at[0, 0], ssem.at[22])
        await_bytes(arcv.at[0, 0], ssem.at[14])
        await_bytes(st_m.at[0, 0], ssem.at[12])

    @pl.when(c == 1)
    def _():
        await_bytes(l1.at[pl.ds(0, nh)], ssem.at[8])
        await_bytes(st_b.at[:, pl.ds(0, n - 1)], ssem.at[19])
        await_bytes(fin, ssem.at[20])
        await_bytes(rrcv.at[:, :, pl.ds(0, n - 1)], ssem.at[21])
        await_bytes(xbuf.at[pl.ds(0, nx - 1)], ssem.at[15])
        await_bytes(xbuf.at[pl.ds(0, nx - 1)], ssem.at[15])
        await_bytes(xbuf.at[0], ssem.at[16])

    open_scope.close()


def write_out(tg_v, pg_v, tg_o, pg_o, sem):
    parts = 8
    copies = [pltpu.make_async_copy(pg_v, pg_o, sem.at[parts])]
    size = tg_v.shape[0] // parts
    for i in range(parts):
        at = pl.ds(i * size, size)
        copies.append(pltpu.make_async_copy(tg_v.at[at], tg_o.at[at], sem.at[i]))
    for one in copies:
        one.start()
    for one in copies:
        one.wait()


def per_device(n, nx, tokens, logits, slot_grad, phi_param):
    tokens, logits, slot_grad = tokens[0], logits[0], slot_grad[0]
    ts, d = tokens.shape
    sl = logits.shape[1] // 2
    rows = d // (n * n)
    gs = slot_grad.shape[0]
    half = d // 2
    tile = min(256, ts)
    vm, dma = pltpu.VMEM, pltpu.SemaphoreType.DMA
    any_spec = pl.BlockSpec(memory_space=pl.ANY)
    scratch = [
        vm((2, ts, d), BF16), vm((d, 2 * ts), BF16), vm((2, ts, sl), BF16),
        vm((2, ts, sl), F32), vm((2, ts, sl), F32), vm((2 * ts, sl), BF16),
        vm((ts, 4 * sl), BF16), vm((4 * sl, d), BF16), vm((d, sl), F32),
        vm((gs, half), BF16), vm((rows // 2, sl), BF16),
        vm((n, 2, gs, half), BF16), vm((2, n // 2, n, 2, gs, half), BF16),
        vm((n, n, 2, rows // 2, sl), BF16),
        vm((n, 4, sl), F32), vm((2, n, 4, sl), F32), vm((2, n, 4, sl), F32),
        vm((2, 4, sl), F32), vm((2, 4, sl), F32),
        vm((n, n * rows, sl), BF16), vm((2, n, n * rows, sl), BF16),
        vm((n, n * rows, sl), BF16), vm((2, n, n * rows, sl), BF16),
        vm((2, n * rows, sl), F32), vm((d, 2 * sl), BF16),
        vm((2, 2, n, rows, sl), F32), vm((2, 2, n, rows, sl), F32),
        vm((2, rows // 2, 2 * sl), F32), vm((nx, rows // 2, 2 * sl), F32),
        vm((ts, sl), F32), vm((ts, sl), F32), vm((2, 4, sl), F32),
        dma((6,)), dma((29,)), dma((27,)), dma((n // 2,)),
    ]
    vm_spec = pl.BlockSpec(memory_space=pltpu.VMEM)
    token_grad, phi_grad = pl.pallas_call(
        functools.partial(kernel, n, nx),
        out_shape=(pltpu.VMEM((ts, d), BF16), pltpu.VMEM((rows // 2, 2 * sl), F32)),
        in_specs=[any_spec] * 4,
        out_specs=(vm_spec, vm_spec),
        scratch_shapes=scratch,
        compiler_params=pltpu.CompilerParams(
            collective_id=0, has_side_effects=True, vmem_limit_bytes=56000000
        ),
        name="moe_dispatch_backward",
    )(tokens, logits, slot_grad, phi_param)
    token_grad, phi_grad = pl.pallas_call(
        write_out,
        out_shape=(
            jax.ShapeDtypeStruct((ts, d), BF16),
            jax.ShapeDtypeStruct((rows // 2, 2 * sl), F32),
        ),
        in_specs=[any_spec, any_spec],
        out_specs=(any_spec, any_spec),
        scratch_shapes=[dma((9,))],
        compiler_params=pltpu.CompilerParams(vmem_limit_bytes=4 * 1024 * 1024),
        name="write_out",
    )(token_grad, phi_grad)
    return token_grad[None], phi_grad


def solution(mesh):
    count, nx = mesh.devices.shape
    n = round((count // 2) ** 0.5)
    finer = Mesh(mesh.devices.reshape(n, n, 2, nx), (*SEQ, "batch"))
    in_specs = (P("batch", SEQ, None), P("batch", SEQ, None), P("batch", SEQ, None), P(SEQ, None))
    out_specs = (P("batch", SEQ, None), P(SEQ, None))
    return jax.shard_map(
        functools.partial(per_device, n, nx),
        mesh=finer, in_specs=in_specs, out_specs=out_specs, check_vma=False,
    )
```
